256 devices in a mesh: wide: 64 (over x, z, core), narrow: 4 (over y).
Axes of the slice: x: 4, y: 4, z: 8, core: 2. Of those that a mesh axis runs over, the one named last changes fastest.
Arguments:
- a_blocks: float32 [49152, 128, 128], P(('wide', 'narrow')), may hold values from -0.8 to 0.8
- row_map: int32 [49152, 128], P(('wide', 'narrow')), may hold values from 0 to 127
- col_map: int32 [49152, 128], P(('wide', 'narrow')), may hold values from 0 to 127
- target: int32 [49152], P(('wide', 'narrow')), may hold values from 0 to 839
- counts: int32 [64], P('wide'), may hold values from 1 to 8, as said below
- weights: int32 [512], P('wide'), may hold values from 1 to 999
Outputs:
- coarse: float32 [512, 128, 128], P('wide', 'narrow')
- work_offset: int32 [512], P('wide')
The draws below stay inside these ranges and needn't reach their ends.
Inputs may be any that keep to these rules, and one draw needn't show every extreme that they name: `counts`: every index of wide has at least one live slot and at most 8; some index has exactly 8; the last index has fewer than 8.
All inputs are finite; a program needn't handle non-finite values.
Results may differ from the reference program's by a relative error of at most 0.0003.
Values sent between devices are 32-bit elements; how exact they have to be, the bound alone decides.
A program may use at most 128 MiB of HBM per device.

```python
import jax
import jax.numpy as jnp
from jax import lax

BS = 128
NB_DEV = 192
S_DEV = 8
BLOCKS = 49152
COARSE = 512
N_WIDE = 64
N_NARROW = 4


def draw_counts(key, part):
    first, second, third = jax.random.split(jax.random.fold_in(key, 17), 3)
    exponent = jax.random.randint(first, (N_WIDE,), 0, 4)
    ceiling = jnp.minimum(jnp.left_shift(1, exponent), S_DEV)
    positions = jnp.arange(N_WIDE)
    ceiling = jnp.where(positions == N_WIDE - 1, jnp.minimum(ceiling, S_DEV - 1), ceiling)
    values = 1 + jax.random.randint(second, (N_WIDE,), 0, 840) % ceiling
    chosen = jax.random.randint(third, (), 0, N_WIDE - 1)
    values = jnp.where(positions == chosen, S_DEV, values)
    return values.astype(jnp.int32)


def touch_ends(values, key, low, high):
    place = [jax.random.randint(jax.random.fold_in(key, axis), (), 0, length) for axis, length in enumerate(values.shape)]
    longest = values.shape.index(max(values.shape))
    next_to = place[:longest] + [(place[longest] + 1) % values.shape[longest]] + place[longest + 1:]
    return values.at[tuple(place)].set(low).at[tuple(next_to)].set(high)


def level_of(rng, dims, cuts, low, largest):
    level = 1.0
    for dim, parts in cuts:
        steps = jax.random.uniform(jax.random.fold_in(jax.random.fold_in(rng, 6), dim), (parts,), jnp.float32, low / len(cuts), largest / len(cuts))
        level = level * jnp.repeat(jnp.exp(steps), dims[dim] // parts).reshape((-1,) + (1,) * (len(dims) - 1 - dim))
    return level


def noise(rng, shape, width, reach, shards=(), held_as=jnp.bfloat16):
    values = jax.random.normal(rng, shape, jnp.float32) * width
    if len(shards) > 0:
        values = level_of(rng, shape, shards, -0.22, 0.18) * values
    return jnp.clip(values, min=-reach, max=reach).astype(held_as)


def setup_inputs(seed: int = 0) -> dict:
    key_list = jax.random.split(jax.random.key(seed), 7)
    a_blocks = noise(key_list[0], (BLOCKS, BS, BS), 0.1, 0.8, ((0, 256),), jnp.float32)
    row_map = touch_ends(jax.random.randint(key_list[1], (BLOCKS, BS), 0, BS), jax.random.fold_in(key_list[1], 1), 0, BS - 1).astype(jnp.int32)
    col_map = touch_ends(jax.random.randint(key_list[2], (BLOCKS, BS), 0, BS), jax.random.fold_in(key_list[2], 1), 0, BS - 1).astype(jnp.int32)
    target = touch_ends(jax.random.randint(key_list[3], (BLOCKS,), 0, 840), jax.random.fold_in(key_list[3], 1), 0, 839).astype(jnp.int32)
    counts = draw_counts(jax.random.fold_in(key_list[6], 71), 0)
    weights = touch_ends(jax.random.randint(key_list[5], (COARSE,), 1, 1000), jax.random.fold_in(key_list[5], 1), 1, 999).astype(jnp.int32)
    return dict(a_blocks=a_blocks, row_map=row_map, col_map=col_map, target=target, counts=counts, weights=weights)


def reference(a_blocks, row_map, col_map, target, counts, weights):
    per_row = NB_DEV * N_NARROW
    slot_of = (target.reshape(N_WIDE, per_row) % counts[:, None]).astype(jnp.int32)

    def one_row(pieces):
        entries, rows_of, cols_of, slots_here = pieces
        index = (slots_here[:, None, None] * BS + rows_of[:, :, None]) * BS + cols_of[:, None, :]
        sums = jax.ops.segment_sum(entries.reshape(-1), index.reshape(-1).astype(jnp.int32), num_segments=S_DEV * BS * BS)
        return sums.reshape(S_DEV, BS, BS)

    partial_value = lax.map(one_row, (a_blocks.reshape(N_WIDE, per_row, BS, BS), row_map.reshape(N_WIDE, per_row, BS), col_map.reshape(N_WIDE, per_row, BS), slot_of))
    target_positions = jnp.arange(S_DEV, dtype=jnp.int32)
    is_live = target_positions[None, :] < counts[:, None]
    suffix_total = jnp.cumsum(counts[::-1])[::-1].astype(jnp.int32)
    start = (COARSE - suffix_total).astype(jnp.int32)
    global_index = jnp.where(is_live, start[:, None] + target_positions[None, :], COARSE).astype(jnp.int32).reshape(-1)
    coarse = jnp.zeros((COARSE, BS, BS), jnp.float32).at[global_index].set(partial_value.reshape(COARSE, BS, BS), mode="drop")
    live_weight = jnp.where(is_live, weights.reshape(N_WIDE, S_DEV), 0).astype(jnp.int32).reshape(-1)
    after = (jnp.cumsum(live_weight[::-1])[::-1] - live_weight).astype(jnp.int32)
    work_offset = jnp.zeros((COARSE,), jnp.int32).at[global_index].set(after, mode="drop")
    return coarse, work_offset
```

```python
import functools

import jax
import jax.numpy as jnp
from jax import lax
from jax.experimental import pallas as pl
from jax.experimental.pallas import tpu as pltpu
from jax.sharding import PartitionSpec as P

BLOCK = 128
GROUP = 16


def split(value):
    high = value.astype(jnp.bfloat16)
    return high, (value - high.astype(jnp.float32)).astype(jnp.bfloat16)


def reduced_block(a, row, col, sublane):
    one, zero = jnp.float32(1), jnp.float32(0)
    pick_row = jnp.where(sublane == row, one, zero).astype(jnp.bfloat16)
    pick_col = jnp.where(sublane == col, one, zero).astype(jnp.bfloat16)
    merged = jnp.dot(
        jnp.concatenate([pick_row, pick_row], 1),
        jnp.concatenate(split(a), 0),
        preferred_element_type=jnp.float32,
    )
    return lax.dot_general(
        jnp.concatenate(split(merged), 1),
        jnp.concatenate([pick_col, pick_col], 1),
        (((1,), (1,)), ((), ())),
        preferred_element_type=jnp.float32,
    )


def partial_kernel(target, counts, a_hbm, row_map, col_map, out, a_vmem, arrived):
    steps = a_hbm.shape[0] // GROUP

    def copy(i):
        part = pl.ds(i * GROUP, GROUP)
        return pltpu.make_async_copy(a_hbm.at[part], a_vmem.at[part], arrived.at[i])

    for i in range(steps):
        copy(i).start()
    out[...] = jnp.zeros_like(out)
    live = counts[0]
    sublane = lax.broadcasted_iota(jnp.int32, (BLOCK, BLOCK), 0)

    def step(i, carry):
        copy(i).wait()
        for j in range(GROUP):
            b = i * GROUP + j
            out[lax.rem(target[b], live)] += reduced_block(
                a_vmem[b], row_map[pl.ds(b, 1), :], col_map[pl.ds(b, 1), :], sublane
            )
        return carry

    lax.fori_loop(0, steps, step, 0)


def partial_sums(a_blocks, row_map, col_map, target, counts, slots):
    n = a_blocks.shape[0]
    smem = pl.BlockSpec(memory_space=pltpu.SMEM)
    vmem = pl.BlockSpec(memory_space=pltpu.VMEM)
    return pl.pallas_call(
        partial_kernel,
        out_shape=jax.ShapeDtypeStruct((slots, BLOCK, BLOCK), jnp.float32),
        in_specs=[smem, smem, pl.BlockSpec(memory_space=pl.ANY), vmem, vmem],
        out_specs=vmem,
        scratch_shapes=[
            pltpu.VMEM((n, BLOCK, BLOCK), jnp.float32),
            pltpu.SemaphoreType.DMA((n // GROUP,)),
        ],
        cost_estimate=pl.CostEstimate(flops=n * 8 * BLOCK**3, bytes_accessed=n * BLOCK * BLOCK * 4, transcendentals=0),
        name="partial_sums",
    )(target, counts, a_blocks, row_map, col_map)


def from_everyone(array, axis):
    devices = lax.axis_size(axis)
    return lax.all_to_all(
        jnp.broadcast_to(array[None], (devices, *array.shape)), axis, 0, 0, tiled=True
    )


def collected_together(array, axis):
    leaves = jax.tree.leaves(array)
    turns = sorted(range(len(leaves)), key=lambda k: -leaves[k].size)
    width = (1, *leaves[turns[0]].shape)[-1]
    lines = [
        jnp.pad(leaves[k].reshape(-1), (0, -leaves[k].size % width)).reshape(-1, width)
        for k in turns
    ]
    both, at, found = (from_everyone(jnp.concatenate(lines), axis), 0, {})
    for k, line in zip(turns, lines):
        piece = both[:, at : at + len(line)].reshape(len(both), -1)
        found[k] = piece[:, : leaves[k].size].reshape(-1, *leaves[k].shape)
        at += len(line)
    numbers = iter(range(len(leaves)))
    return jax.tree.map(lambda _: found[next(numbers)], array)


def folded_in_pairs(pieces, combine):
    while len(jax.tree.leaves(pieces)[0]) > 1:
        pieces = jax.vmap(combine)(
            *(jax.tree.map(lambda part: part[side::2], pieces) for side in (0, 1))
        )
    return jax.tree.map(lambda part: part[0], pieces)


def entering(array, axis, combine, identity):
    devices, place = (lax.axis_size(axis), lax.axis_index(axis))
    passed = jnp.arange(devices) > place

    def kept(part, zero, own):
        part = jnp.where(
            passed.reshape(-1, *(1 for _ in own.shape)), part, jnp.asarray(zero, own.dtype)
        )
        return part[::-1]

    pieces = collected_together(array, axis)
    return folded_in_pairs(jax.tree.map(kept, pieces, identity, array), combine)


def cut_along(array, dim, devices):
    shape = array.shape
    pieces = array.reshape(*shape[:dim], devices, shape[dim] // devices, *shape[dim + 1 :])
    return jnp.moveaxis(pieces, dim, 0)


def summed_on_arrival(array, axis, dim):
    pieces = cut_along(array, dim, lax.axis_size(axis))
    arrived = lax.all_to_all(pieces, axis, split_axis=0, concat_axis=0, tiled=True)
    return arrived.sum(axis=0)


def local(a_blocks, row_map, col_map, target, counts, weights):
    slot_count = weights.shape[0]
    nwide = lax.axis_size("wide")
    own_index = lax.axis_index("wide")
    live_count = counts[0]
    target_positions = jnp.arange(slot_count, dtype=jnp.int32)
    is_live = target_positions < live_count
    live_weight = jnp.where(is_live, weights, 0)
    local_total = jnp.sum(live_weight)

    def combine(earlier, later):
        return (earlier[0] + later[0], earlier[1] + later[1])

    zero_one = jnp.zeros((1,), jnp.int32)
    higher_count, higher_weight = entering(
        (counts, local_total[None]), "wide", combine, (zero_one, zero_one)
    )
    higher_count = higher_count[0]
    higher_weight = higher_weight[0]
    start = (nwide * slot_count - higher_count - live_count).astype(jnp.int32)
    partial_value = partial_sums(a_blocks, row_map, col_map, target, counts, slot_count)
    accumulated_sum = summed_on_arrival(partial_value, "narrow", 1)
    destination = jnp.where(is_live, start + target_positions, -1)
    offset_of = jnp.where(is_live, higher_weight + local_total - jnp.cumsum(live_weight), 0).astype(
        jnp.int32
    )

    def place(carry, piece, first_row):
        blocks_in, entry_index, offset_in = piece
        local_position = entry_index - own_index * slot_count
        pick = local_position[None, :] == target_positions[:, None]
        blocks_acc = jnp.einsum(
            "sk,kjm->sjm", pick.astype(jnp.float32), blocks_in, precision=lax.Precision.HIGHEST
        )
        offset_acc = jnp.sum(jnp.where(pick, offset_in[None, :], 0), axis=1).astype(jnp.int32)
        return (blocks_acc, offset_acc)

    starting_value = (jnp.zeros_like(accumulated_sum), jnp.zeros((slot_count,), jnp.int32))
    coarse, work_offset = place(
        starting_value,
        (
            lax.all_gather(accumulated_sum, "wide", axis=0, tiled=True),
            lax.all_gather(destination, "wide", axis=0, tiled=True),
            lax.all_gather(offset_of, "wide", axis=0, tiled=True),
        ),
        jnp.int32(0),
    )
    return (coarse, work_offset)


def solution(mesh):
    return jax.shard_map(
        local,
        mesh=mesh,
        in_specs=(
            P(("wide", "narrow"), None, None),
            P(("wide", "narrow"), None),
            P(("wide", "narrow"), None),
            P(("wide", "narrow")),
            P("wide"),
            P("wide"),
        ),
        out_specs=(P("wide", "narrow", None), P("wide")),
        check_vma=False,
    )
```

```python
import functools

import jax
import jax.numpy as jnp
from jax import lax
from jax.experimental import pallas as pl
from jax.experimental.pallas import tpu as pltpu
from jax.sharding import PartitionSpec as P

BLOCK = 128
GROUP = 16
SLOTS = 8
WIDE = 64
NARROW = 4
CHIPS = WIDE // 2
Z = 8
X = CHIPS // Z
ROWS = BLOCK // NARROW
HALF = SLOTS // 2
F32 = jnp.float32
I32 = jnp.int32
BF16 = jnp.bfloat16


def split(value):
    high = value.astype(BF16)
    return high, (value - high.astype(F32)).astype(BF16)


def reduced_block(a, row, col, sublane):
    one, zero = F32(1), F32(0)
    pick_row = jnp.where(sublane == row, one, zero).astype(BF16)
    pick_col = jnp.where(sublane == col, one, zero).astype(BF16)
    merged = jnp.dot(
        jnp.concatenate([pick_row, pick_row], 1),
        jnp.concatenate(split(a), 0),
        preferred_element_type=F32,
    )
    return lax.dot_general(
        jnp.concatenate(split(merged), 1),
        jnp.concatenate([pick_col, pick_col], 1),
        (((1,), (1,)), ((), ())),
        preferred_element_type=F32,
    )


def partial_kernel(target, counts, a_hbm, row_map, col_map, out, a_vmem, arrived):
    steps = a_hbm.shape[0] // GROUP

    def copy(i):
        part = pl.ds(i * GROUP, GROUP)
        return pltpu.make_async_copy(a_hbm.at[part], a_vmem.at[part], arrived.at[i])

    for i in range(steps):
        copy(i).start()
    out[...] = jnp.zeros_like(out)
    live = counts[0]
    sublane = lax.broadcasted_iota(I32, (BLOCK, BLOCK), 0)

    def step(i, carry):
        copy(i).wait()
        for j in range(GROUP):
            b = i * GROUP + j
            out[lax.rem(target[b], live)] += reduced_block(
                a_vmem[b], row_map[pl.ds(b, 1), :], col_map[pl.ds(b, 1), :], sublane
            )
        return carry

    lax.fori_loop(0, steps, step, 0)


def partial_sums(a_blocks, row_map, col_map, target, counts):
    n = a_blocks.shape[0]
    smem = pl.BlockSpec(memory_space=pltpu.SMEM)
    vmem = pl.BlockSpec(memory_space=pltpu.VMEM)
    return pl.pallas_call(
        partial_kernel,
        out_shape=jax.ShapeDtypeStruct((SLOTS, BLOCK, BLOCK), F32),
        in_specs=[smem, smem, pl.BlockSpec(memory_space=pl.ANY), vmem, vmem],
        out_specs=vmem,
        scratch_shapes=[
            pltpu.VMEM((n, BLOCK, BLOCK), F32),
            pltpu.SemaphoreType.DMA((n // GROUP,)),
        ],
        name="partial_sums",
    )(target, counts, a_blocks, row_map, col_map)


def place_kernel(
    counts, weights, partial, coarse, offset,
    meta_own, meta, via_up, via_down, send_up, send_down, from_down, from_up,
    rows_out, rows_in, pick, placed, back, note_own, note_in,
    y_sent, y_got, meta_sent, meta_got, out_sent, out_got, back_sent, back_got, note_sent, note_got,
):
    w = lax.axis_index("wide")
    y = lax.axis_index("narrow")
    core = lax.rem(w, 2)
    chip = lax.div(w, 2)
    x = lax.div(chip, Z)
    z = lax.rem(chip, Z)
    up, down = lax.rem(y + 1, NARROW), lax.rem(y + NARROW - 1, NARROW)
    far = lax.rem(y + 2, NARROW)

    def remote(src, dst, sent, got, wide, narrow):
        return pltpu.make_async_remote_copy(
            src_ref=src, dst_ref=dst, send_sem=sent, recv_sem=got,
            device_id={"wide": wide, "narrow": narrow},
            device_id_type=pl.DeviceIdType.MESH,
        )

    barrier = pltpu.get_barrier_semaphore()
    for other in (up, down):
        pl.semaphore_signal(barrier, inc=1, device_id={"wide": w, "narrow": other},
                            device_id_type=pl.DeviceIdType.MESH)

    def greet(d, carry):
        pl.semaphore_signal(barrier, inc=1, device_id={"wide": lax.rem(w + d, WIDE), "narrow": y},
                            device_id_type=pl.DeviceIdType.MESH)
        return carry

    lax.fori_loop(1, WIDE, greet, 0)

    lane = lax.broadcasted_iota(I32, (1, BLOCK), 1)
    turn = lax.rem(lane, SLOTS)
    weight_row = jnp.zeros((1, BLOCK), I32)
    for s in range(SLOTS):
        weight_row = jnp.where(turn == s, weights[s], weight_row)
    meta_own[:, :BLOCK] = jnp.full((1, BLOCK), counts[0], I32)
    meta_own[:, BLOCK:] = weight_row
    pl.semaphore_wait(barrier, WIDE + 1)

    def piece(half, owner):
        return partial.at[pl.ds(half * HALF, HALF), pl.ds(owner * ROWS, ROWS), :]

    def y_copy(k):
        src, dst, narrow = (
            (piece(0, far), via_up, up),
            (piece(1, far), via_down, down),
            (piece(1, up), from_down.at[pl.ds(HALF, HALF)], up),
            (piece(0, down), from_up.at[pl.ds(0, HALF)], down),
            (send_up, from_down.at[pl.ds(0, HALF)], up),
            (send_down, from_up.at[pl.ds(HALF, HALF)], down),
        )[k]
        return remote(src, dst, y_sent.at[k], y_got.at[k], w, narrow)

    for k in range(4):
        y_copy(k).start()

    def each_chip(body):
        def visit(d, carry):
            dx = lax.rem(X // 2 + lax.div(d, Z), X)
            dz = lax.rem(Z // 2 + lax.rem(d, Z), Z)
            there = lax.rem(x + dx, X) * Z + lax.rem(z + dz, Z)

            @pl.when((there != chip) | (core == 0))
            def _():
                body(there)

            return carry

        lax.fori_loop(0, CHIPS, visit, 0)

    each_chip(lambda there: remote(
        meta_own, meta.at[w], meta_sent, meta_got, 2 * there + 1, y).start())

    y_copy(0).wait_recv()
    send_up[...] = via_up[...] + partial[pl.ds(0, HALF), pl.ds(up * ROWS, ROWS), :]
    y_copy(4).start()
    y_copy(1).wait_recv()
    send_down[...] = via_down[...] + partial[pl.ds(HALF, HALF), pl.ds(down * ROWS, ROWS), :]
    y_copy(5).start()

    @pl.when(core == 1)
    def _():
        meta[w] = meta_own[...]
        remote(meta.at[pl.ds(0, WIDE - 1)], meta.at[pl.ds(0, WIDE - 1)], meta_sent, meta_got, w - 1, y).wait_recv()
        total = WIDE * SLOTS
        entry = lax.broadcasted_iota(I32, (WIDE, total), 1)
        device = lax.broadcasted_iota(I32, (WIDE, total), 0)
        count = jnp.concatenate([meta[:, 0, :BLOCK]] * (total // BLOCK), 1).astype(F32)
        weight = jnp.concatenate([meta[:, 0, BLOCK:]] * (total // BLOCK), 1).astype(F32)
        owner = lax.div(entry, SLOTS)
        mine = device == owner
        zero = jnp.zeros_like(count)
        count_row = jnp.sum(jnp.where(mine, count, zero), 0, keepdims=True)
        weight_of = jnp.sum(jnp.where(mine, weight, zero), 0, keepdims=True)
        higher = jnp.sum(jnp.where(device >= owner, count, zero), 0, keepdims=True)
        slot = lax.rem(lax.broadcasted_iota(I32, (1, total), 1), SLOTS).astype(F32)
        live = slot < count_row
        goes_to = jnp.where(live, F32(total) - higher + slot, F32(-1))
        first = F32(total) - jnp.max(higher, 1, keepdims=True)
        wide_rows = lax.broadcasted_iota(I32, (total, total), 0).astype(F32)
        pick[...] = jnp.where(wide_rows == goes_to, F32(1), F32(0)).astype(BF16)
        for k in range(2):
            index = (lax.broadcasted_iota(I32, (SLOTS, total), 0) + (2 * chip + k) * SLOTS).astype(F32)
            above = jnp.sum(jnp.where(goes_to > index, weight_of, F32(0)), 1, keepdims=True)
            above = jnp.where(index[:, :1] >= first, above, F32(0))
            diagonal = lax.broadcasted_iota(I32, (SLOTS, BLOCK), 0) == lax.broadcasted_iota(I32, (SLOTS, BLOCK), 1)
            line = jnp.sum(jnp.where(diagonal, above, F32(0)), 0, keepdims=True).astype(I32)
            if k == 0:
                note_own[...] = line
            else:
                offset[...] = line[:, :SLOTS]
        note = remote(note_own, note_in, note_sent, note_got, w - 1, y)
        note.start()

    for k in (2, 3, 4, 5):
        y_copy(k).wait_recv()
    for s in range(SLOTS):
        rows_out[:, s, :] = (
            partial[s, pl.ds(y * ROWS, ROWS), :] + from_down[s] + from_up[s]
        )

    each_chip(lambda there: remote(
        rows_out.at[there], rows_in.at[w], out_sent, out_got, 2 * there + 1, y).start())

    @pl.when(core == 1)
    def _():
        rows_in[w] = rows_out[chip]
        most = rows_in.at[pl.ds(0, WIDE - 1)]
        remote(most, most, out_sent, out_got, w - 1, y).wait_recv()
        high, low = split(rows_in[...].reshape(WIDE * SLOTS, BLOCK))
        both = jnp.dot(pick[...], jnp.concatenate([high, low], 1), preferred_element_type=F32)
        placed[...] = (both[:, :BLOCK] + both[:, BLOCK:]).reshape(WIDE, SLOTS, BLOCK)
        back[chip] = placed[w]

        def deliver(d, carry):
            there = lax.rem(w + d, WIDE)
            remote(placed.at[there], back.at[chip], back_sent, back_got, there, y).start()
            return carry

        lax.fori_loop(1, WIDE, deliver, 0)
        few = back.at[pl.ds(0, CHIPS - 1)]
        remote(few, few, back_sent, back_got, w - 1, y).wait_recv()

    @pl.when(core == 0)
    def _():
        remote(back, back, back_sent, back_got, w + 1, y).wait_recv()
        remote(note_in, note_in, note_sent, note_got, w + 1, y).wait_recv()
        offset[...] = note_in[:, :SLOTS]

    for s in range(SLOTS):
        coarse[s] = back[:, s, :]

    for k in range(6):
        y_copy(k).wait_send()

    @pl.when(core == 1)
    def _():
        remote(note_own, note_in, note_sent, note_got, w - 1, y).wait_send()
        most = placed.at[pl.ds(0, WIDE - 1)]
        remote(most, most, back_sent, back_got, w - 1, y).wait_send()
        few = rows_out.at[pl.ds(0, CHIPS - 1)]
        remote(few, few, out_sent, out_got, w - 1, y).wait_send()
        some = meta.at[pl.ds(0, CHIPS - 1)]
        remote(some, some, meta_sent, meta_got, w - 1, y).wait_send()

    @pl.when(core == 0)
    def _():
        remote(rows_out, rows_out, out_sent, out_got, w + 1, y).wait_send()
        some = meta.at[pl.ds(0, CHIPS)]
        remote(some, some, meta_sent, meta_got, w + 1, y).wait_send()


def placed_blocks(counts, weights, partial):
    smem = pl.BlockSpec(memory_space=pltpu.SMEM)
    vmem = pl.BlockSpec(memory_space=pltpu.VMEM)
    dma = pltpu.SemaphoreType.DMA
    return pl.pallas_call(
        place_kernel,
        out_shape=(
            jax.ShapeDtypeStruct((SLOTS, ROWS, BLOCK), F32),
            jax.ShapeDtypeStruct((1, SLOTS), I32),
        ),
        in_specs=[smem, smem, vmem],
        out_specs=(vmem, vmem),
        scratch_shapes=[
            pltpu.VMEM((1, 2 * BLOCK), I32),
            pltpu.VMEM((WIDE, 1, 2 * BLOCK), I32),
            pltpu.VMEM((HALF, ROWS, BLOCK), F32),
            pltpu.VMEM((HALF, ROWS, BLOCK), F32),
            pltpu.VMEM((HALF, ROWS, BLOCK), F32),
            pltpu.VMEM((HALF, ROWS, BLOCK), F32),
            pltpu.VMEM((SLOTS, ROWS, BLOCK), F32),
            pltpu.VMEM((SLOTS, ROWS, BLOCK), F32),
            pltpu.VMEM((CHIPS, SLOTS, BLOCK), F32),
            pltpu.VMEM((WIDE, SLOTS, BLOCK), F32),
            pltpu.VMEM((WIDE * SLOTS, WIDE * SLOTS), BF16),
            pltpu.VMEM((WIDE, SLOTS, BLOCK), F32),
            pltpu.VMEM((CHIPS, SLOTS, BLOCK), F32),
            pltpu.VMEM((1, BLOCK), I32),
            pltpu.VMEM((1, BLOCK), I32),
            dma((6,)), dma((6,)),
            dma, dma, dma, dma, dma, dma, dma, dma,
        ],
        compiler_params=pltpu.CompilerParams(collective_id=0, has_side_effects=True),
        name="placed_blocks",
    )(counts, weights, partial)


def local(a_blocks, row_map, col_map, target, counts, weights):
    partial = partial_sums(a_blocks, row_map, col_map, target, counts)
    coarse, offset = placed_blocks(counts, weights, partial)
    return coarse, offset.reshape(SLOTS)


def solution(mesh):
    return jax.shard_map(
        local,
        mesh=mesh,
        in_specs=(
            P(("wide", "narrow"), None, None),
            P(("wide", "narrow"), None),
            P(("wide", "narrow"), None),
            P(("wide", "narrow")),
            P("wide"),
            P("wide"),
        ),
        out_specs=(P("wide", "narrow", None), P("wide")),
        check_vma=False,
    )
```

```python
import functools

import jax
import jax.numpy as jnp
from jax import lax
from jax.experimental import pallas as pl
from jax.experimental.pallas import tpu as pltpu
from jax.sharding import PartitionSpec as P

BLOCK = 128
GROUP = 32
SLOTS = 8
WIDE = 64
NARROW = 4
CHIPS = WIDE // 2
Z = 8
X = CHIPS // Z
ROWS = BLOCK // NARROW
HALF = SLOTS // 2
FINE = 192
PADDED = 256
UNIT = 4
STEP = 6
RUNS = (FINE + SLOTS * (UNIT - 1)) // UNIT
VMEM_LIMIT = 48 * 2**20
F32 = jnp.float32
I32 = jnp.int32
BF16 = jnp.bfloat16


def split(value):
    high = value.astype(BF16)
    return high, (value - high.astype(F32)).astype(BF16)


def reduced_block(a, row, col, sublane):
    one, zero = F32(1), F32(0)
    pick_row = jnp.where(sublane == row, one, zero).astype(BF16)
    pick_col = jnp.where(sublane == col, one, zero).astype(BF16)
    merged = jnp.dot(
        jnp.concatenate([pick_row, pick_row], 1),
        jnp.concatenate(split(a), 0),
        preferred_element_type=F32,
    )
    return lax.dot_general(
        jnp.concatenate(split(merged), 1),
        jnp.concatenate([pick_col, pick_col], 1),
        (((1,), (1,)), ((), ())),
        preferred_element_type=F32,
    )


def order_table(target, live):
    padded = (PADDED, PADDED)
    one, zero = jnp.ones(padded, F32), jnp.zeros(padded, F32)
    code = target.astype(F32)
    count = jnp.full((1, FINE), jnp.maximum(live, 1), I32).astype(F32)
    slot = code - jnp.floor((code + 0.5) / count) * count
    slot = jnp.concatenate([slot, jnp.full((1, PADDED - FINE), SLOTS, F32)], 1)
    lane = lax.broadcasted_iota(I32, padded, 1)
    sublane = lax.broadcasted_iota(I32, padded, 0)
    across = jnp.broadcast_to(slot, padded)
    down = jnp.sum(jnp.where(lane == sublane, across, zero), 1, keepdims=True)
    place = jnp.sum(jnp.where((across == down) & (lane < sublane), one, zero), 1, keepdims=True)
    place = jnp.where(down == SLOTS, F32(1e6), place)
    column = lax.broadcasted_iota(I32, (1, PADDED), 1)
    base = jnp.zeros((1, 1), F32)
    keep = jnp.ones((1, PADDED), F32)
    last = jnp.zeros((1, PADDED), F32)
    for s in range(SLOTS):
        size = jnp.sum(jnp.where(slot == s, F32(1), F32(0)), 1, keepdims=True)
        runs = jnp.floor((size + (UNIT - 1)) * (1.0 / UNIT))
        place = place + jnp.where(down == s, base * UNIT, F32(0))
        keep = jnp.where((column.astype(F32) == base) & (size > 0), F32(0), keep)
        last = jnp.where(column == s, jnp.where(size > 0, base + runs - 1, F32(RUNS)), last)
        base = base + runs
    found = jnp.where(place == lane.astype(F32), sublane.astype(F32) + 1, zero)
    found = jnp.sum(found, 0, keepdims=True)
    source = jnp.where(found > 0, found - 1, F32(FINE))
    return jnp.concatenate([source, keep, last, jnp.zeros((5, PADDED), F32)], 0).astype(I32)


def coarse_kernel(
    counts, weights_hbm, target_hbm, row_hbm, col_hbm, a_hbm, back, note_out,
    weights, target, a_vmem, row_map, col_map, reduced, run_sums, table, order, partial,
    meta_own, meta, via_up, via_down, send_up, send_down, from_down, from_up,
    rows_out, rows_in, pick, placed, note_own, note_in,
    a_got, map_got, order_got,
    y_sent, y_got, meta_sent, meta_got, out_sent, out_got, back_sent, back_got, note_sent, note_got,
):
    steps = FINE // GROUP

    def a_copy(i):
        part = pl.ds(i * GROUP, GROUP)
        return pltpu.make_async_copy(a_hbm.at[part], a_vmem.at[part], a_got.at[i])

    row_copy = pltpu.make_async_copy(row_hbm, row_map, map_got.at[0])
    col_copy = pltpu.make_async_copy(col_hbm, col_map, map_got.at[1])
    small_copies = [
        pltpu.make_async_copy(src, dst, map_got.at[2 + k])
        for k, (src, dst) in enumerate(
            ((target_hbm, target), (weights_hbm, weights))
        )
    ]
    for copy in small_copies:
        copy.start()
    row_copy.start()
    col_copy.start()
    for i in range(steps):
        a_copy(i).start()

    w = lax.axis_index("wide")
    y = lax.axis_index("narrow")
    core = lax.rem(w, 2)
    chip = lax.div(w, 2)
    x = lax.div(chip, Z)
    z = lax.rem(chip, Z)
    up, down = lax.rem(y + 1, NARROW), lax.rem(y + NARROW - 1, NARROW)
    far = lax.rem(y + 2, NARROW)

    def remote(src, dst, sent, got, wide, narrow):
        return pltpu.make_async_remote_copy(
            src_ref=src, dst_ref=dst, send_sem=sent, recv_sem=got,
            device_id={"wide": wide, "narrow": narrow},
            device_id_type=pl.DeviceIdType.MESH,
        )

    barrier = pltpu.get_barrier_semaphore()
    for other in (up, down):
        pl.semaphore_signal(barrier, inc=1, device_id={"wide": w, "narrow": other},
                            device_id_type=pl.DeviceIdType.MESH)

    def greet(d, carry):
        pl.semaphore_signal(barrier, inc=1, device_id={"wide": lax.rem(w + d, WIDE), "narrow": y},
                            device_id_type=pl.DeviceIdType.MESH)
        return carry

    lax.fori_loop(1, WIDE, greet, 0)

    for copy in small_copies:
        copy.wait()
    lane = lax.broadcasted_iota(I32, (1, BLOCK), 1)
    turn = lax.rem(lane, SLOTS)
    weight_row = jnp.zeros((1, BLOCK), I32)
    for s in range(SLOTS):
        weight_row = jnp.where(turn == s, weights[s], weight_row)
    meta_own[:, :BLOCK] = jnp.full((1, BLOCK), counts[0], I32)
    meta_own[:, BLOCK:] = weight_row

    def piece(half, owner):
        return partial.at[pl.ds(half * HALF, HALF), pl.ds(owner * ROWS, ROWS), :]

    def y_copy(k):
        src, dst, narrow = (
            (piece(0, far), via_up, up),
            (piece(1, far), via_down, down),
            (piece(1, up), from_down.at[pl.ds(HALF, HALF)], up),
            (piece(0, down), from_up.at[pl.ds(0, HALF)], down),
            (send_up, from_down.at[pl.ds(0, HALF)], up),
            (send_down, from_up.at[pl.ds(HALF, HALF)], down),
        )[k]
        return remote(src, dst, y_sent.at[k], y_got.at[k], w, narrow)

    near = [lax.rem(z + Z // 2 + k, Z) for k in range(Z)]

    def each_chip(body):
        def visit(d, carry):
            base = lax.rem(x + X // 2 + d, X) * Z
            for k in range(Z):
                body(base + near[k])
            return carry

        lax.fori_loop(0, X, visit, 0)

    def to_rows(send):
        def body(there):
            @pl.when((there != chip) | (core == 0))
            def _():
                send(there).start()

        each_chip(body)

    table[...] = order_table(target[...], counts[0])
    order_copy = pltpu.make_async_copy(table, order, order_got)
    order_copy.start()
    reduced[FINE] = jnp.zeros((BLOCK, BLOCK), F32)
    run_sums[RUNS] = jnp.zeros((BLOCK, BLOCK), F32)
    sublane = lax.broadcasted_iota(I32, (BLOCK, BLOCK), 0)

    def reduce_group(i, carry):
        @pl.when(i == steps - 2)
        def _():
            pl.semaphore_wait(barrier, WIDE + 1)
            to_rows(lambda there: remote(
                meta_own, meta.at[w], meta_sent, meta_got, 2 * there + 1, y))

        a_copy(i).wait()
        for j in range(GROUP):
            b = i * GROUP + j
            reduced[b] = reduced_block(
                a_vmem[b], row_map[pl.ds(b, 1), :], col_map[pl.ds(b, 1), :], sublane
            )
        return carry

    row_copy.wait()
    col_copy.wait()
    lax.fori_loop(0, steps, reduce_group, 0)
    order_copy.wait()

    def add_runs(i, total):
        for k in range(STEP):
            run = i * STEP + k
            total = total * order[1, run].astype(F32)
            for u in range(UNIT):
                total = total + reduced[jnp.clip(order[0, run * UNIT + u], 0, FINE)]
            run_sums[run] = total
        return total

    lax.fori_loop(0, RUNS // STEP, add_runs, jnp.zeros((BLOCK, BLOCK), F32))
    for s in range(SLOTS):
        partial[s] = run_sums[jnp.clip(order[2, s], 0, RUNS)]

    for k in range(4):
        y_copy(k).start()

    y_copy(0).wait_recv()
    send_up[...] = via_up[...] + partial[pl.ds(0, HALF), pl.ds(up * ROWS, ROWS), :]
    y_copy(4).start()
    y_copy(1).wait_recv()
    send_down[...] = via_down[...] + partial[pl.ds(HALF, HALF), pl.ds(down * ROWS, ROWS), :]
    y_copy(5).start()

    @pl.when(core == 1)
    def _():
        meta[w] = meta_own[...]
        remote(meta.at[pl.ds(0, WIDE - 1)], meta.at[pl.ds(0, WIDE - 1)], meta_sent, meta_got, w - 1, y).wait_recv()
        total = WIDE * SLOTS
        entry = lax.broadcasted_iota(I32, (WIDE, total), 1)
        device = lax.broadcasted_iota(I32, (WIDE, total), 0)
        count = jnp.concatenate([meta[:, 0, :BLOCK]] * (total // BLOCK), 1).astype(F32)
        weight = jnp.concatenate([meta[:, 0, BLOCK:]] * (total // BLOCK), 1).astype(F32)
        owner = lax.div(entry, SLOTS)
        mine = device == owner
        zero = jnp.zeros_like(count)
        count_row = jnp.sum(jnp.where(mine, count, zero), 0, keepdims=True)
        weight_of = jnp.sum(jnp.where(mine, weight, zero), 0, keepdims=True)
        higher = jnp.sum(jnp.where(device >= owner, count, zero), 0, keepdims=True)
        slot = lax.rem(lax.broadcasted_iota(I32, (1, total), 1), SLOTS).astype(F32)
        live = slot < count_row
        goes_to = jnp.where(live, F32(total) - higher + slot, F32(-1))
        first = F32(total) - jnp.max(higher, 1, keepdims=True)
        wide_rows = lax.broadcasted_iota(I32, (total, total), 0).astype(F32)
        pick[...] = jnp.where(wide_rows == goes_to, F32(1), F32(0)).astype(BF16)
        for k in range(2):
            index = (lax.broadcasted_iota(I32, (SLOTS, total), 0) + (2 * chip + k) * SLOTS).astype(F32)
            above = jnp.sum(jnp.where(goes_to > index, weight_of, F32(0)), 1, keepdims=True)
            above = jnp.where(index[:, :1] >= first, above, F32(0))
            diagonal = lax.broadcasted_iota(I32, (SLOTS, BLOCK), 0) == lax.broadcasted_iota(I32, (SLOTS, BLOCK), 1)
            line = jnp.sum(jnp.where(diagonal, above, F32(0)), 0, keepdims=True).astype(I32)
            if k == 0:
                note_own[...] = line
            else:
                note_out[...] = line
        note = remote(note_own, note_in, note_sent, note_got, w - 1, y)
        note.start()

    for k in (2, 3, 4, 5):
        y_copy(k).wait_recv()
    for s in range(SLOTS):
        rows_out[:, s, :] = (
            partial[s, pl.ds(y * ROWS, ROWS), :] + from_down[s] + from_up[s]
        )

    to_rows(lambda there: remote(
        rows_out.at[there], rows_in.at[w], out_sent, out_got, 2 * there + 1, y))

    @pl.when(core == 1)
    def _():
        rows_in[w] = rows_out[chip]
        most = rows_in.at[pl.ds(0, WIDE - 1)]
        remote(most, most, out_sent, out_got, w - 1, y).wait_recv()
        high, low = split(rows_in[...].reshape(WIDE * SLOTS, BLOCK))
        both = jnp.dot(pick[...], jnp.concatenate([high, low], 1), preferred_element_type=F32)
        placed[...] = (both[:, :BLOCK] + both[:, BLOCK:]).reshape(WIDE, SLOTS, BLOCK)
        back[chip] = placed[w]

        def deliver(there):
            remote(placed.at[2 * there], back.at[chip], back_sent, back_got, 2 * there, y).start()

            @pl.when(there != chip)
            def _():
                remote(placed.at[2 * there + 1], back.at[chip], back_sent, back_got, 2 * there + 1, y).start()

        each_chip(deliver)
        few = back.at[pl.ds(0, CHIPS - 1)]
        remote(few, few, back_sent, back_got, w - 1, y).wait_recv()

    @pl.when(core == 0)
    def _():
        remote(back, back, back_sent, back_got, w + 1, y).wait_recv()
        remote(note_in, note_in, note_sent, note_got, w + 1, y).wait_recv()
        note_out[...] = note_in[...]

    for k in range(6):
        y_copy(k).wait_send()

    @pl.when(core == 1)
    def _():
        remote(note_own, note_in, note_sent, note_got, w - 1, y).wait_send()
        most = placed.at[pl.ds(0, WIDE - 1)]
        remote(most, most, back_sent, back_got, w - 1, y).wait_send()
        few = rows_out.at[pl.ds(0, CHIPS - 1)]
        remote(few, few, out_sent, out_got, w - 1, y).wait_send()
        some = meta.at[pl.ds(0, CHIPS - 1)]
        remote(some, some, meta_sent, meta_got, w - 1, y).wait_send()

    @pl.when(core == 0)
    def _():
        remote(rows_out, rows_out, out_sent, out_got, w + 1, y).wait_send()
        some = meta.at[pl.ds(0, CHIPS)]
        remote(some, some, meta_sent, meta_got, w + 1, y).wait_send()


def finish_kernel(back, note, coarse, offset):
    for s in range(SLOTS):
        coarse[s] = back[:, s, :]
    offset[...] = note[:, :SLOTS]


def local(a_blocks, row_map, col_map, target, counts, weights):
    vmem = pl.BlockSpec(memory_space=pltpu.VMEM)
    hbm = pl.BlockSpec(memory_space=pltpu.HBM)
    dma = pltpu.SemaphoreType.DMA
    half = pltpu.VMEM((HALF, ROWS, BLOCK), F32)
    full = pltpu.VMEM((SLOTS, ROWS, BLOCK), F32)
    plane = pltpu.VMEM((WIDE, SLOTS, BLOCK), F32)
    line = pltpu.VMEM((1, BLOCK), I32)
    back, note = pl.pallas_call(
        coarse_kernel,
        out_shape=(
            jax.ShapeDtypeStruct((CHIPS, SLOTS, BLOCK), F32),
            jax.ShapeDtypeStruct((1, BLOCK), I32),
        ),
        in_specs=[pl.BlockSpec(memory_space=pltpu.SMEM)] + [hbm] * 5,
        out_specs=(vmem, vmem),
        scratch_shapes=[
            pltpu.SMEM((SLOTS,), I32),
            pltpu.VMEM((1, FINE), I32),
            pltpu.VMEM((FINE, BLOCK, BLOCK), F32),
            pltpu.VMEM((FINE, BLOCK), I32),
            pltpu.VMEM((FINE, BLOCK), I32),
            pltpu.VMEM((FINE + 1, BLOCK, BLOCK), F32),
            pltpu.VMEM((RUNS + 1, BLOCK, BLOCK), F32),
            pltpu.VMEM((8, PADDED), I32),
            pltpu.SMEM((8, PADDED), I32),
            pltpu.VMEM((SLOTS, BLOCK, BLOCK), F32),
            pltpu.VMEM((1, 2 * BLOCK), I32),
            pltpu.VMEM((WIDE, 1, 2 * BLOCK), I32),
            half, half, half, half, full, full,
            pltpu.VMEM((CHIPS, SLOTS, BLOCK), F32),
            plane,
            pltpu.VMEM((WIDE * SLOTS, WIDE * SLOTS), BF16),
            plane,
            line, line,
            dma((FINE // GROUP,)), dma((4,)), dma,
            dma((6,)), dma((6,)),
            dma, dma, dma, dma, dma, dma, dma, dma,
        ],
        compiler_params=pltpu.CompilerParams(
            collective_id=0, has_side_effects=True, vmem_limit_bytes=VMEM_LIMIT
        ),
        name="coarse_blocks",
    )(counts, *(pltpu.with_memory_space_constraint(each, pltpu.HBM) for each in (
        weights, target.reshape(1, FINE), row_map, col_map, a_blocks)))
    coarse, offset = pl.pallas_call(
        finish_kernel,
        out_shape=(
            jax.ShapeDtypeStruct((SLOTS, ROWS, BLOCK), F32),
            jax.ShapeDtypeStruct((1, SLOTS), I32),
        ),
        in_specs=[vmem, vmem],
        out_specs=(vmem, vmem),
        compiler_params=pltpu.CompilerParams(vmem_limit_bytes=4 * 2**20),
        name="finish",
    )(back, note)
    return coarse, offset.reshape(SLOTS)


def solution(mesh):
    return jax.shard_map(
        local,
        mesh=mesh,
        in_specs=(
            P(("wide", "narrow"), None, None),
            P(("wide", "narrow"), None),
            P(("wide", "narrow"), None),
            P(("wide", "narrow")),
            P("wide"),
            P("wide"),
        ),
        out_specs=(P("wide", "narrow", None), P("wide")),
        check_vma=False,
    )
```

```python
import functools

import jax
import jax.numpy as jnp
from jax import lax
from jax.experimental import pallas as pl
from jax.experimental.pallas import tpu as pltpu
from jax.sharding import PartitionSpec as P

BLOCK = 128
GROUP = 32
SLOTS = 8
WIDE = 64
NARROW = 4
CHIPS = WIDE // 2
Z = 8
X = CHIPS // Z
ROWS = BLOCK // NARROW
HALF = SLOTS // 2
FINE = 192
PADDED = 256
UNIT = 4
STEP = 18
RUNS = (FINE + SLOTS * (UNIT - 1)) // UNIT
VMEM_LIMIT = 48 * 2**20
F32 = jnp.float32
I32 = jnp.int32
BF16 = jnp.bfloat16


def split(value):
    high = value.astype(BF16)
    return high, (value - high.astype(F32)).astype(BF16)


def merged_block(a, col, sublane):
    chosen = picked(col, sublane)
    merged = lax.dot_general(
        jnp.concatenate(split(a), 1),
        jnp.concatenate([chosen, chosen], 1),
        (((1,), (1,)), ((), ())),
        preferred_element_type=F32,
    )
    return jnp.concatenate(split(merged), 1)


def picked(index, sublane):
    return jnp.where(sublane == index, F32(1), F32(0)).astype(BF16)


def order_table(target, live):
    padded = (PADDED, PADDED)
    one, zero = jnp.ones(padded, F32), jnp.zeros(padded, F32)
    code = target.astype(F32)
    count = jnp.full((1, FINE), jnp.maximum(live, 1), I32).astype(F32)
    slot = code - jnp.floor((code + 0.5) / count) * count
    slot = jnp.concatenate([slot, jnp.full((1, PADDED - FINE), SLOTS, F32)], 1)
    lane = lax.broadcasted_iota(I32, padded, 1)
    sublane = lax.broadcasted_iota(I32, padded, 0)
    across = jnp.broadcast_to(slot, padded)
    down = jnp.sum(jnp.where(lane == sublane, across, zero), 1, keepdims=True)
    place = jnp.sum(jnp.where((across == down) & (lane < sublane), one, zero), 1, keepdims=True)
    place = jnp.where(down == SLOTS, F32(1e6), place)
    column = lax.broadcasted_iota(I32, (1, PADDED), 1)
    base = jnp.zeros((1, 1), F32)
    keep = jnp.ones((1, PADDED), F32)
    last = jnp.zeros((1, PADDED), F32)
    for s in range(SLOTS):
        size = jnp.sum(jnp.where(slot == s, F32(1), F32(0)), 1, keepdims=True)
        runs = jnp.floor((size + (UNIT - 1)) * (1.0 / UNIT))
        place = place + jnp.where(down == s, base * UNIT, F32(0))
        keep = jnp.where((column.astype(F32) == base) & (size > 0), F32(0), keep)
        last = jnp.where(column == s, jnp.where(size > 0, base + runs - 1, F32(RUNS)), last)
        base = base + runs
    found = jnp.where(place == lane.astype(F32), sublane.astype(F32) + 1, zero)
    found = jnp.sum(found, 0, keepdims=True)
    source = jnp.where(found > 0, found - 1, F32(FINE))
    return jnp.concatenate([source, keep, last, jnp.zeros((5, PADDED), F32)], 0).astype(I32)


def coarse_kernel(
    counts, weights_hbm, target_hbm, row_hbm, col_hbm, a_hbm, back, note_out,
    weights, target, a_vmem, row_map, col_map, merged, run_sums, table, order, partial,
    meta_own, meta, via_up, via_down, send_up, send_down, from_down, from_up,
    rows_out, rows_in, pick, placed, note_own, note_in,
    a_got, map_got, order_got,
    y_sent, y_got, meta_sent, meta_got, out_sent, out_got, back_sent, back_got, note_sent, note_got,
):
    steps = FINE // GROUP

    def a_copy(i):
        part = pl.ds(i * GROUP, GROUP)
        return pltpu.make_async_copy(a_hbm.at[part], a_vmem.at[part], a_got.at[i])

    row_copy = pltpu.make_async_copy(row_hbm, row_map.at[pl.ds(0, FINE)], map_got.at[0])
    col_copy = pltpu.make_async_copy(col_hbm, col_map, map_got.at[1])
    small_copies = [
        pltpu.make_async_copy(src, dst, map_got.at[2 + k])
        for k, (src, dst) in enumerate(
            ((target_hbm, target), (weights_hbm, weights))
        )
    ]
    for copy in small_copies:
        copy.start()
    row_copy.start()
    col_copy.start()
    for i in range(steps):
        a_copy(i).start()

    w = lax.axis_index("wide")
    y = lax.axis_index("narrow")
    core = lax.rem(w, 2)
    chip = lax.div(w, 2)
    x = lax.div(chip, Z)
    z = lax.rem(chip, Z)
    up, down = lax.rem(y + 1, NARROW), lax.rem(y + NARROW - 1, NARROW)
    far = lax.rem(y + 2, NARROW)

    def remote(src, dst, sent, got, wide, narrow):
        return pltpu.make_async_remote_copy(
            src_ref=src, dst_ref=dst, send_sem=sent, recv_sem=got,
            device_id={"wide": wide, "narrow": narrow},
            device_id_type=pl.DeviceIdType.MESH,
        )

    barrier = pltpu.get_barrier_semaphore()
    for other in (up, down):
        pl.semaphore_signal(barrier, inc=1, device_id={"wide": w, "narrow": other},
                            device_id_type=pl.DeviceIdType.MESH)

    def greet(d, carry):
        pl.semaphore_signal(barrier, inc=1, device_id={"wide": lax.rem(w + d, WIDE), "narrow": y},
                            device_id_type=pl.DeviceIdType.MESH)
        return carry

    lax.fori_loop(1, WIDE, greet, 0)

    for copy in small_copies:
        copy.wait()
    lane = lax.broadcasted_iota(I32, (1, BLOCK), 1)
    turn = lax.rem(lane, SLOTS)
    weight_row = jnp.zeros((1, BLOCK), I32)
    for s in range(SLOTS):
        weight_row = jnp.where(turn == s, weights[s], weight_row)
    meta_own[:, :BLOCK] = jnp.full((1, BLOCK), counts[0], I32)
    meta_own[:, BLOCK:] = weight_row

    def piece(half, owner):
        return partial.at[pl.ds(half * HALF, HALF), pl.ds(owner * ROWS, ROWS), :]

    def y_copy(k):
        src, dst, narrow = (
            (piece(0, far), via_up, up),
            (piece(1, far), via_down, down),
            (piece(1, up), from_down.at[pl.ds(HALF, HALF)], up),
            (piece(0, down), from_up.at[pl.ds(0, HALF)], down),
            (send_up, from_down.at[pl.ds(0, HALF)], up),
            (send_down, from_up.at[pl.ds(HALF, HALF)], down),
        )[k]
        return remote(src, dst, y_sent.at[k], y_got.at[k], w, narrow)

    near = [lax.rem(z + Z // 2 + k, Z) for k in range(Z)]

    def each_chip(body):
        def visit(d, carry):
            base = lax.rem(x + X // 2 + d, X) * Z
            for k in range(Z):
                body(base + near[k])
            return carry

        lax.fori_loop(0, X, visit, 0)

    def to_rows(send):
        def body(there):
            @pl.when((there != chip) | (core == 0))
            def _():
                send(there).start()

        each_chip(body)

    table[...] = order_table(target[...], counts[0])
    order_copy = pltpu.make_async_copy(table, order, order_got)
    order_copy.start()
    merged[FINE] = jnp.zeros((BLOCK, 2 * BLOCK), BF16)
    row_map[pl.ds(FINE, SLOTS), :] = jnp.zeros((SLOTS, BLOCK), I32)
    run_sums[RUNS] = jnp.zeros((BLOCK, BLOCK), F32)
    sublane = lax.broadcasted_iota(I32, (BLOCK, BLOCK), 0)

    def reduce_group(i, carry):
        @pl.when(i == steps - 2)
        def _():
            pl.semaphore_wait(barrier, WIDE + 1)
            to_rows(lambda there: remote(
                meta_own, meta.at[w], meta_sent, meta_got, 2 * there + 1, y))

        a_copy(i).wait()
        for j in range(GROUP):
            b = i * GROUP + j
            merged[b] = merged_block(a_vmem[b], col_map[pl.ds(b, 1), :], sublane)
        return carry

    col_copy.wait()
    lax.fori_loop(0, steps, reduce_group, 0)
    row_copy.wait()
    order_copy.wait()

    def add_runs(i, total):
        for k in range(STEP):
            run = i * STEP + k
            at = [jnp.clip(order[0, run * UNIT + u], 0, FINE) for u in range(UNIT)]
            added = jnp.dot(
                jnp.concatenate([picked(row_map[pl.ds(b, 1), :], sublane) for b in at], 1),
                jnp.concatenate([merged[b] for b in at], 0),
                preferred_element_type=F32,
            )
            added = added[:, :BLOCK] + added[:, BLOCK:]
            total = total * order[1, run].astype(F32) + added
            run_sums[run] = total
        return total

    lax.fori_loop(0, RUNS // STEP, add_runs, jnp.zeros((BLOCK, BLOCK), F32))
    for s in range(SLOTS):
        partial[s] = run_sums[jnp.clip(order[2, s], 0, RUNS)]

    for k in range(4):
        y_copy(k).start()

    y_copy(0).wait_recv()
    send_up[...] = via_up[...] + partial[pl.ds(0, HALF), pl.ds(up * ROWS, ROWS), :]
    y_copy(4).start()
    y_copy(1).wait_recv()
    send_down[...] = via_down[...] + partial[pl.ds(HALF, HALF), pl.ds(down * ROWS, ROWS), :]
    y_copy(5).start()

    @pl.when(core == 1)
    def _():
        meta[w] = meta_own[...]
        remote(meta.at[pl.ds(0, WIDE - 1)], meta.at[pl.ds(0, WIDE - 1)], meta_sent, meta_got, w - 1, y).wait_recv()
        total = WIDE * SLOTS
        entry = lax.broadcasted_iota(I32, (WIDE, total), 1)
        device = lax.broadcasted_iota(I32, (WIDE, total), 0)
        count = jnp.concatenate([meta[:, 0, :BLOCK]] * (total // BLOCK), 1).astype(F32)
        weight = jnp.concatenate([meta[:, 0, BLOCK:]] * (total // BLOCK), 1).astype(F32)
        owner = lax.div(entry, SLOTS)
        mine = device == owner
        zero = jnp.zeros_like(count)
        count_row = jnp.sum(jnp.where(mine, count, zero), 0, keepdims=True)
        weight_of = jnp.sum(jnp.where(mine, weight, zero), 0, keepdims=True)
        higher = jnp.sum(jnp.where(device >= owner, count, zero), 0, keepdims=True)
        slot = lax.rem(lax.broadcasted_iota(I32, (1, total), 1), SLOTS).astype(F32)
        live = slot < count_row
        goes_to = jnp.where(live, F32(total) - higher + slot, F32(-1))
        first = F32(total) - jnp.max(higher, 1, keepdims=True)
        wide_rows = lax.broadcasted_iota(I32, (total, total), 0).astype(F32)
        pick[...] = jnp.where(wide_rows == goes_to, F32(1), F32(0)).astype(BF16)
        for k in range(2):
            index = (lax.broadcasted_iota(I32, (SLOTS, total), 0) + (2 * chip + k) * SLOTS).astype(F32)
            above = jnp.sum(jnp.where(goes_to > index, weight_of, F32(0)), 1, keepdims=True)
            above = jnp.where(index[:, :1] >= first, above, F32(0))
            diagonal = lax.broadcasted_iota(I32, (SLOTS, BLOCK), 0) == lax.broadcasted_iota(I32, (SLOTS, BLOCK), 1)
            line = jnp.sum(jnp.where(diagonal, above, F32(0)), 0, keepdims=True).astype(I32)
            if k == 0:
                note_own[...] = line
            else:
                note_out[...] = line
        note = remote(note_own, note_in, note_sent, note_got, w - 1, y)
        note.start()

    for k in (2, 3, 4, 5):
        y_copy(k).wait_recv()
    for s in range(SLOTS):
        rows_out[:, s, :] = (
            partial[s, pl.ds(y * ROWS, ROWS), :] + from_down[s] + from_up[s]
        )

    to_rows(lambda there: remote(
        rows_out.at[there], rows_in.at[w], out_sent, out_got, 2 * there + 1, y))

    @pl.when(core == 1)
    def _():
        rows_in[w] = rows_out[chip]
        most = rows_in.at[pl.ds(0, WIDE - 1)]
        remote(most, most, out_sent, out_got, w - 1, y).wait_recv()
        high, low = split(rows_in[...].reshape(WIDE * SLOTS, BLOCK))
        both = jnp.dot(pick[...], jnp.concatenate([high, low], 1), preferred_element_type=F32)
        placed[...] = (both[:, :BLOCK] + both[:, BLOCK:]).reshape(WIDE, SLOTS, BLOCK)
        back[chip] = placed[w]

        def deliver(there):
            remote(placed.at[2 * there], back.at[chip], back_sent, back_got, 2 * there, y).start()

            @pl.when(there != chip)
            def _():
                remote(placed.at[2 * there + 1], back.at[chip], back_sent, back_got, 2 * there + 1, y).start()

        each_chip(deliver)
        few = back.at[pl.ds(0, CHIPS - 1)]
        remote(few, few, back_sent, back_got, w - 1, y).wait_recv()

    @pl.when(core == 0)
    def _():
        remote(back, back, back_sent, back_got, w + 1, y).wait_recv()
        remote(note_in, note_in, note_sent, note_got, w + 1, y).wait_recv()
        note_out[...] = note_in[...]

    for k in range(6):
        y_copy(k).wait_send()

    @pl.when(core == 1)
    def _():
        remote(note_own, note_in, note_sent, note_got, w - 1, y).wait_send()
        most = placed.at[pl.ds(0, WIDE - 1)]
        remote(most, most, back_sent, back_got, w - 1, y).wait_send()
        few = rows_out.at[pl.ds(0, CHIPS - 1)]
        remote(few, few, out_sent, out_got, w - 1, y).wait_send()
        some = meta.at[pl.ds(0, CHIPS - 1)]
        remote(some, some, meta_sent, meta_got, w - 1, y).wait_send()

    @pl.when(core == 0)
    def _():
        remote(rows_out, rows_out, out_sent, out_got, w + 1, y).wait_send()
        some = meta.at[pl.ds(0, CHIPS)]
        remote(some, some, meta_sent, meta_got, w + 1, y).wait_send()


def finish_kernel(back, note, coarse, offset):
    for s in range(SLOTS):
        coarse[s] = back[:, s, :]
    offset[...] = note[:, :SLOTS]


def local(a_blocks, row_map, col_map, target, counts, weights):
    vmem = pl.BlockSpec(memory_space=pltpu.VMEM)
    hbm = pl.BlockSpec(memory_space=pltpu.HBM)
    dma = pltpu.SemaphoreType.DMA
    half = pltpu.VMEM((HALF, ROWS, BLOCK), F32)
    full = pltpu.VMEM((SLOTS, ROWS, BLOCK), F32)
    plane = pltpu.VMEM((WIDE, SLOTS, BLOCK), F32)
    line = pltpu.VMEM((1, BLOCK), I32)
    back, note = pl.pallas_call(
        coarse_kernel,
        out_shape=(
            jax.ShapeDtypeStruct((CHIPS, SLOTS, BLOCK), F32),
            jax.ShapeDtypeStruct((1, BLOCK), I32),
        ),
        in_specs=[pl.BlockSpec(memory_space=pltpu.SMEM)] + [hbm] * 5,
        out_specs=(vmem, vmem),
        scratch_shapes=[
            pltpu.SMEM((SLOTS,), I32),
            pltpu.VMEM((1, FINE), I32),
            pltpu.VMEM((FINE, BLOCK, BLOCK), F32),
            pltpu.VMEM((FINE + SLOTS, BLOCK), I32),
            pltpu.VMEM((FINE, BLOCK), I32),
            pltpu.VMEM((FINE + 1, BLOCK, 2 * BLOCK), BF16),
            pltpu.VMEM((RUNS + 1, BLOCK, BLOCK), F32),
            pltpu.VMEM((8, PADDED), I32),
            pltpu.SMEM((8, PADDED), I32),
            pltpu.VMEM((SLOTS, BLOCK, BLOCK), F32),
            pltpu.VMEM((1, 2 * BLOCK), I32),
            pltpu.VMEM((WIDE, 1, 2 * BLOCK), I32),
            half, half, half, half, full, full,
            pltpu.VMEM((CHIPS, SLOTS, BLOCK), F32),
            plane,
            pltpu.VMEM((WIDE * SLOTS, WIDE * SLOTS), BF16),
            plane,
            line, line,
            dma((FINE // GROUP,)), dma((4,)), dma,
            dma((6,)), dma((6,)),
            dma, dma, dma, dma, dma, dma, dma, dma,
        ],
        compiler_params=pltpu.CompilerParams(
            collective_id=0, has_side_effects=True, vmem_limit_bytes=VMEM_LIMIT
        ),
        name="coarse_blocks",
    )(counts, *(pltpu.with_memory_space_constraint(each, pltpu.HBM) for each in (
        weights, target.reshape(1, FINE), row_map, col_map, a_blocks)))
    coarse, offset = pl.pallas_call(
        finish_kernel,
        out_shape=(
            jax.ShapeDtypeStruct((SLOTS, ROWS, BLOCK), F32),
            jax.ShapeDtypeStruct((1, SLOTS), I32),
        ),
        in_specs=[vmem, vmem],
        out_specs=(vmem, vmem),
        compiler_params=pltpu.CompilerParams(vmem_limit_bytes=4 * 2**20),
        name="finish",
    )(back, note)
    return coarse, offset.reshape(SLOTS)


def solution(mesh):
    return jax.shard_map(
        local,
        mesh=mesh,
        in_specs=(
            P(("wide", "narrow"), None, None),
            P(("wide", "narrow"), None),
            P(("wide", "narrow"), None),
            P(("wide", "narrow")),
            P("wide"),
            P("wide"),
        ),
        out_specs=(P("wide", "narrow", None), P("wide")),
        check_vma=False,
    )
```

```python
import functools

import jax
import jax.numpy as jnp
from jax import lax
from jax.experimental import pallas as pl
from jax.experimental.pallas import tpu as pltpu
from jax.sharding import PartitionSpec as P

BLOCK = 128
GROUP = 24
SLOTS = 8
WIDE = 64
NARROW = 4
CHIPS = WIDE // 2
Z = 8
X = CHIPS // Z
ROWS = BLOCK // NARROW
HALF = SLOTS // 2
FINE = 192
PADDED = 256
UNIT = 4
STEP = 27
AHEAD = 3
RUNS = (FINE + SLOTS * (UNIT - 1)) // UNIT
VMEM_LIMIT = 48 * 2**20
F32 = jnp.float32
I32 = jnp.int32
BF16 = jnp.bfloat16


def split(value):
    high = value.astype(BF16)
    return high, (value - high.astype(F32)).astype(BF16)


def merged_block(a, col, sublane):
    chosen = picked(col, sublane)
    merged = lax.dot_general(
        jnp.concatenate(split(a), 1),
        jnp.concatenate([chosen, chosen], 1),
        (((1,), (1,)), ((), ())),
        preferred_element_type=F32,
    )
    return jnp.concatenate(split(merged), 1)


def picked(index, sublane):
    return jnp.where(sublane == index, F32(1), F32(0)).astype(BF16)


def order_table(target, live):
    padded = (PADDED, PADDED)
    one, zero = jnp.ones(padded, F32), jnp.zeros(padded, F32)
    code = target.astype(F32)
    count = jnp.full((1, FINE), jnp.maximum(live, 1), I32).astype(F32)
    slot = code - jnp.floor((code + 0.5) / count) * count
    slot = jnp.concatenate([slot, jnp.full((1, PADDED - FINE), SLOTS, F32)], 1)
    lane = lax.broadcasted_iota(I32, padded, 1)
    sublane = lax.broadcasted_iota(I32, padded, 0)
    across = jnp.broadcast_to(slot, padded)
    down = jnp.sum(jnp.where(lane == sublane, across, zero), 1, keepdims=True)
    place = jnp.sum(jnp.where((across == down) & (lane < sublane), one, zero), 1, keepdims=True)
    place = jnp.where(down == SLOTS, F32(1e6), place)
    column = lax.broadcasted_iota(I32, (1, PADDED), 1)
    base = jnp.zeros((1, 1), F32)
    keep = jnp.ones((1, PADDED), F32)
    last = jnp.zeros((1, PADDED), F32)
    for s in range(SLOTS):
        size = jnp.sum(jnp.where(slot == s, F32(1), F32(0)), 1, keepdims=True)
        runs = jnp.floor((size + (UNIT - 1)) * (1.0 / UNIT))
        place = place + jnp.where(down == s, base * UNIT, F32(0))
        keep = jnp.where((column.astype(F32) == base) & (size > 0), F32(0), keep)
        last = jnp.where(column == s, jnp.where(size > 0, base + runs - 1, F32(RUNS)), last)
        base = base + runs
    found = jnp.where(place == lane.astype(F32), sublane.astype(F32) + 1, zero)
    found = jnp.sum(found, 0, keepdims=True)
    source = jnp.where(found > 0, found - 1, F32(FINE))
    return jnp.concatenate([source, keep, last, jnp.zeros((5, PADDED), F32)], 0).astype(I32)


def coarse_kernel(
    counts, weights_hbm, target_hbm, row_hbm, col_hbm, a_hbm, back, note_out,
    weights, target, a_vmem, row_map, col_map, merged, run_sums, table, order, partial,
    meta_own, meta, via_up, via_down, send_up, send_down, from_down, from_up,
    rows_out, rows_in, pick, placed, note_own, note_in,
    a_got, map_got, order_got,
    y_sent, y_got, meta_sent, meta_got, out_sent, out_got, back_sent, back_got, note_sent, note_got,
):
    steps = FINE // GROUP

    def a_copy(i):
        part = pl.ds(i * GROUP, GROUP)
        return pltpu.make_async_copy(a_hbm.at[part], a_vmem.at[part], a_got.at[i])

    row_copy = pltpu.make_async_copy(row_hbm, row_map.at[pl.ds(0, FINE)], map_got.at[0])
    col_copy = pltpu.make_async_copy(col_hbm, col_map, map_got.at[1])
    small_copies = [
        pltpu.make_async_copy(src, dst, map_got.at[2 + k])
        for k, (src, dst) in enumerate(
            ((target_hbm, target), (weights_hbm, weights))
        )
    ]
    a_copy(0).start()
    for copy in small_copies:
        copy.start()
    col_copy.start()

    w = lax.axis_index("wide")
    y = lax.axis_index("narrow")
    core = lax.rem(w, 2)
    chip = lax.div(w, 2)
    x = lax.div(chip, Z)
    z = lax.rem(chip, Z)
    up, down = lax.rem(y + 1, NARROW), lax.rem(y + NARROW - 1, NARROW)
    far = lax.rem(y + 2, NARROW)

    def remote(src, dst, sent, got, wide, narrow):
        return pltpu.make_async_remote_copy(
            src_ref=src, dst_ref=dst, send_sem=sent, recv_sem=got,
            device_id={"wide": wide, "narrow": narrow},
            device_id_type=pl.DeviceIdType.MESH,
        )

    barrier = pltpu.get_barrier_semaphore()
    for other in (up, down):
        pl.semaphore_signal(barrier, inc=1, device_id={"wide": w, "narrow": other},
                            device_id_type=pl.DeviceIdType.MESH)

    def piece(half, owner):
        return partial.at[pl.ds(half * HALF, HALF), pl.ds(owner * ROWS, ROWS), :]

    def y_copy(k):
        src, dst, narrow = (
            (piece(0, far), via_up, up),
            (piece(1, far), via_down, down),
            (piece(1, up), from_down.at[pl.ds(HALF, HALF)], up),
            (piece(0, down), from_up.at[pl.ds(0, HALF)], down),
            (send_up, from_down.at[pl.ds(0, HALF)], up),
            (send_down, from_up.at[pl.ds(HALF, HALF)], down),
        )[k]
        return remote(src, dst, y_sent.at[k], y_got.at[k], w, narrow)

    near = [lax.rem(z + Z // 2 + k, Z) for k in range(Z)]

    def each_chip(body):
        def visit(d, carry):
            base = lax.rem(x + X // 2 + d, X) * Z
            for k in range(Z):
                body(base + near[k])
            return carry

        lax.fori_loop(0, X, visit, 0)

    def to_rows(send):
        def body(there):
            @pl.when((there != chip) | (core == 0))
            def _():
                send(there).start()

        each_chip(body)

    def greet(there):
        pl.semaphore_signal(barrier, inc=1, device_id={"wide": 2 * there + 1 - core, "narrow": y},
                            device_id_type=pl.DeviceIdType.MESH)

        @pl.when(there != chip)
        def _():
            pl.semaphore_signal(barrier, inc=1, device_id={"wide": 2 * there + core, "narrow": y},
                                device_id_type=pl.DeviceIdType.MESH)

    each_chip(greet)
    row_copy.start()
    for i in range(1, AHEAD):
        a_copy(i).start()
    for copy in small_copies:
        copy.wait()
    lane = lax.broadcasted_iota(I32, (1, BLOCK), 1)
    turn = lax.rem(lane, SLOTS)
    weight_row = jnp.zeros((1, BLOCK), I32)
    for s in range(SLOTS):
        weight_row = jnp.where(turn == s, weights[s], weight_row)
    meta_own[:, :BLOCK] = jnp.full((1, BLOCK), counts[0], I32)
    meta_own[:, BLOCK:] = weight_row

    table[...] = order_table(target[...], counts[0])
    order_copy = pltpu.make_async_copy(table, order, order_got)
    order_copy.start()
    merged[FINE] = jnp.zeros((BLOCK, 2 * BLOCK), BF16)
    row_map[pl.ds(FINE, SLOTS), :] = jnp.zeros((SLOTS, BLOCK), I32)
    run_sums[RUNS] = jnp.zeros((BLOCK, BLOCK), F32)
    sublane = lax.broadcasted_iota(I32, (BLOCK, BLOCK), 0)

    def reduce_group(i, carry):
        a_copy(i).wait()

        @pl.when(i + AHEAD < steps)
        def _():
            a_copy(i + AHEAD).start()

        for j in range(GROUP):
            b = i * GROUP + j
            merged[b] = merged_block(a_vmem[b], col_map[pl.ds(b, 1), :], sublane)
        return carry

    col_copy.wait()
    lax.fori_loop(0, steps, reduce_group, 0)
    row_copy.wait()
    order_copy.wait()

    def add_runs(i, total):
        for k in range(STEP):
            run = i * STEP + k
            at = [jnp.clip(order[0, run * UNIT + u], 0, FINE) for u in range(UNIT)]
            added = jnp.dot(
                jnp.concatenate([picked(row_map[pl.ds(b, 1), :], sublane) for b in at], 1),
                jnp.concatenate([merged[b] for b in at], 0),
                preferred_element_type=F32,
            )
            added = added[:, :BLOCK] + added[:, BLOCK:]
            total = total * order[1, run].astype(F32) + added
            run_sums[run] = total
        return total

    lax.fori_loop(0, RUNS // STEP, add_runs, jnp.zeros((BLOCK, BLOCK), F32))
    for s in range(SLOTS):
        partial[s] = run_sums[jnp.clip(order[2, s], 0, RUNS)]

    pl.semaphore_wait(barrier, WIDE + 1)
    for k in range(4):
        y_copy(k).start()
    to_rows(lambda there: remote(
        meta_own, meta.at[w], meta_sent, meta_got, 2 * there + 1, y))

    y_copy(0).wait_recv()
    send_up[...] = via_up[...] + partial[pl.ds(0, HALF), pl.ds(up * ROWS, ROWS), :]
    y_copy(4).start()
    y_copy(1).wait_recv()
    send_down[...] = via_down[...] + partial[pl.ds(HALF, HALF), pl.ds(down * ROWS, ROWS), :]
    y_copy(5).start()

    for k in (2, 3, 4, 5):
        y_copy(k).wait_recv()
    for s in range(SLOTS):
        rows_out[:, s, :] = (
            partial[s, pl.ds(y * ROWS, ROWS), :] + from_down[s] + from_up[s]
        )

    to_rows(lambda there: remote(
        rows_out.at[there], rows_in.at[w], out_sent, out_got, 2 * there + 1, y))

    @pl.when(core == 1)
    def _():
        rows_in[w] = rows_out[chip]
        meta[w] = meta_own[...]
        remote(meta.at[pl.ds(0, WIDE - 1)], meta.at[pl.ds(0, WIDE - 1)], meta_sent, meta_got, w - 1, y).wait_recv()
        total = WIDE * SLOTS
        entry = lax.broadcasted_iota(I32, (WIDE, total), 1)
        device = lax.broadcasted_iota(I32, (WIDE, total), 0)
        count = jnp.concatenate([meta[:, 0, :BLOCK]] * (total // BLOCK), 1).astype(F32)
        weight = jnp.concatenate([meta[:, 0, BLOCK:]] * (total // BLOCK), 1).astype(F32)
        owner = lax.div(entry, SLOTS)
        mine = device == owner
        zero = jnp.zeros_like(count)
        count_row = jnp.sum(jnp.where(mine, count, zero), 0, keepdims=True)
        weight_of = jnp.sum(jnp.where(mine, weight, zero), 0, keepdims=True)
        higher = jnp.sum(jnp.where(device >= owner, count, zero), 0, keepdims=True)
        slot = lax.rem(lax.broadcasted_iota(I32, (1, total), 1), SLOTS).astype(F32)
        live = slot < count_row
        goes_to = jnp.where(live, F32(total) - higher + slot, F32(-1))
        first = F32(total) - jnp.max(higher, 1, keepdims=True)
        wide_rows = lax.broadcasted_iota(I32, (total, total), 0).astype(F32)
        pick[...] = jnp.where(wide_rows == goes_to, F32(1), F32(0)).astype(BF16)
        for k in range(2):
            index = (lax.broadcasted_iota(I32, (SLOTS, total), 0) + (2 * chip + k) * SLOTS).astype(F32)
            above = jnp.sum(jnp.where(goes_to > index, weight_of, F32(0)), 1, keepdims=True)
            above = jnp.where(index[:, :1] >= first, above, F32(0))
            diagonal = lax.broadcasted_iota(I32, (SLOTS, BLOCK), 0) == lax.broadcasted_iota(I32, (SLOTS, BLOCK), 1)
            line = jnp.sum(jnp.where(diagonal, above, F32(0)), 0, keepdims=True).astype(I32)
            if k == 0:
                note_own[...] = line
            else:
                note_out[...] = line
        note = remote(note_own, note_in, note_sent, note_got, w - 1, y)
        note.start()
        most = rows_in.at[pl.ds(0, WIDE - 1)]
        remote(most, most, out_sent, out_got, w - 1, y).wait_recv()
        high, low = split(rows_in[...].reshape(WIDE * SLOTS, BLOCK))
        both = jnp.dot(pick[...], jnp.concatenate([high, low], 1), preferred_element_type=F32)
        placed[...] = (both[:, :BLOCK] + both[:, BLOCK:]).reshape(WIDE, SLOTS, BLOCK)
        back[chip] = placed[w]

        def deliver(there):
            remote(placed.at[2 * there], back.at[chip], back_sent, back_got, 2 * there, y).start()

            @pl.when(there != chip)
            def _():
                remote(placed.at[2 * there + 1], back.at[chip], back_sent, back_got, 2 * there + 1, y).start()

        each_chip(deliver)
        few = back.at[pl.ds(0, CHIPS - 1)]
        remote(few, few, back_sent, back_got, w - 1, y).wait_recv()

    @pl.when(core == 0)
    def _():
        remote(back, back, back_sent, back_got, w + 1, y).wait_recv()
        remote(note_in, note_in, note_sent, note_got, w + 1, y).wait_recv()
        note_out[...] = note_in[...]

    for k in range(6):
        y_copy(k).wait_send()

    @pl.when(core == 1)
    def _():
        remote(note_own, note_in, note_sent, note_got, w - 1, y).wait_send()
        most = placed.at[pl.ds(0, WIDE - 1)]
        remote(most, most, back_sent, back_got, w - 1, y).wait_send()
        few = rows_out.at[pl.ds(0, CHIPS - 1)]
        remote(few, few, out_sent, out_got, w - 1, y).wait_send()
        some = meta.at[pl.ds(0, CHIPS - 1)]
        remote(some, some, meta_sent, meta_got, w - 1, y).wait_send()

    @pl.when(core == 0)
    def _():
        remote(rows_out, rows_out, out_sent, out_got, w + 1, y).wait_send()
        some = meta.at[pl.ds(0, CHIPS)]
        remote(some, some, meta_sent, meta_got, w + 1, y).wait_send()


def finish_kernel(back, note, coarse, offset):
    for s in range(SLOTS):
        coarse[s] = back[:, s, :]
    offset[...] = note[:, :SLOTS]


def local(a_blocks, row_map, col_map, target, counts, weights):
    vmem = pl.BlockSpec(memory_space=pltpu.VMEM)
    hbm = pl.BlockSpec(memory_space=pltpu.HBM)
    dma = pltpu.SemaphoreType.DMA
    half = pltpu.VMEM((HALF, ROWS, BLOCK), F32)
    full = pltpu.VMEM((SLOTS, ROWS, BLOCK), F32)
    plane = pltpu.VMEM((WIDE, SLOTS, BLOCK), F32)
    line = pltpu.VMEM((1, BLOCK), I32)
    back, note = pl.pallas_call(
        coarse_kernel,
        out_shape=(
            jax.ShapeDtypeStruct((CHIPS, SLOTS, BLOCK), F32),
            jax.ShapeDtypeStruct((1, BLOCK), I32),
        ),
        in_specs=[pl.BlockSpec(memory_space=pltpu.SMEM)] + [hbm] * 5,
        out_specs=(vmem, vmem),
        scratch_shapes=[
            pltpu.SMEM((SLOTS,), I32),
            pltpu.VMEM((1, FINE), I32),
            pltpu.VMEM((FINE, BLOCK, BLOCK), F32),
            pltpu.VMEM((FINE + SLOTS, BLOCK), I32),
            pltpu.VMEM((FINE, BLOCK), I32),
            pltpu.VMEM((FINE + 1, BLOCK, 2 * BLOCK), BF16),
            pltpu.VMEM((RUNS + 1, BLOCK, BLOCK), F32),
            pltpu.VMEM((8, PADDED), I32),
            pltpu.SMEM((8, PADDED), I32),
            pltpu.VMEM((SLOTS, BLOCK, BLOCK), F32),
            pltpu.VMEM((1, 2 * BLOCK), I32),
            pltpu.VMEM((WIDE, 1, 2 * BLOCK), I32),
            half, half, half, half, full, full,
            pltpu.VMEM((CHIPS, SLOTS, BLOCK), F32),
            plane,
            pltpu.VMEM((WIDE * SLOTS, WIDE * SLOTS), BF16),
            plane,
            line, line,
            dma((FINE // GROUP,)), dma((4,)), dma,
            dma((6,)), dma((6,)),
            dma, dma, dma, dma, dma, dma, dma, dma,
        ],
        compiler_params=pltpu.CompilerParams(
            collective_id=0, has_side_effects=True, vmem_limit_bytes=VMEM_LIMIT
        ),
        name="coarse_blocks",
    )(counts, *(pltpu.with_memory_space_constraint(each, pltpu.HBM) for each in (
        weights, target.reshape(1, FINE), row_map, col_map, a_blocks)))
    coarse, offset = pl.pallas_call(
        finish_kernel,
        out_shape=(
            jax.ShapeDtypeStruct((SLOTS, ROWS, BLOCK), F32),
            jax.ShapeDtypeStruct((1, SLOTS), I32),
        ),
        in_specs=[vmem, vmem],
        out_specs=(vmem, vmem),
        compiler_params=pltpu.CompilerParams(vmem_limit_bytes=4 * 2**20),
        name="finish",
    )(back, note)
    return coarse, offset.reshape(SLOTS)


def solution(mesh):
    return jax.shard_map(
        local,
        mesh=mesh,
        in_specs=(
            P(("wide", "narrow"), None, None),
            P(("wide", "narrow"), None),
            P(("wide", "narrow"), None),
            P(("wide", "narrow")),
            P("wide"),
            P("wide"),
        ),
        out_specs=(P("wide", "narrow", None), P("wide")),
        check_vma=False,
    )
```

```python
import functools

import jax
import jax.numpy as jnp
from jax import lax
from jax.experimental import pallas as pl
from jax.experimental.pallas import tpu as pltpu
from jax.sharding import PartitionSpec as P

BLOCK = 128
GROUP = 24
SLOTS = 8
WIDE = 64
NARROW = 4
CHIPS = WIDE // 2
Z = 8
X = CHIPS // Z
ROWS = BLOCK // NARROW
HALF = SLOTS // 2
FINE = 192
PADDED = 256
UNIT = 4
STEP = 27
AHEAD = 3
RUNS = (FINE + SLOTS * (UNIT - 1)) // UNIT
VMEM_LIMIT = 48 * 2**20
F32 = jnp.float32
I32 = jnp.int32
BF16 = jnp.bfloat16


def split(value):
    high = value.astype(BF16)
    return high, (value - high.astype(F32)).astype(BF16)


def merged_block(a, col, sublane):
    chosen = picked(col, sublane)
    merged = lax.dot_general(
        jnp.concatenate(split(a), 1),
        jnp.concatenate([chosen, chosen], 1),
        (((1,), (1,)), ((), ())),
        preferred_element_type=F32,
    )
    return jnp.concatenate(split(merged), 1)


def picked(index, sublane):
    return jnp.where(sublane == index, F32(1), F32(0)).astype(BF16)


def order_table(target, live):
    padded = (PADDED, PADDED)
    one, zero = jnp.ones(padded, F32), jnp.zeros(padded, F32)
    code = target.astype(F32)
    count = jnp.full((1, FINE), jnp.maximum(live, 1), I32).astype(F32)
    slot = code - jnp.floor((code + 0.5) / count) * count
    slot = jnp.concatenate([slot, jnp.full((1, PADDED - FINE), SLOTS, F32)], 1)
    lane = lax.broadcasted_iota(I32, padded, 1)
    sublane = lax.broadcasted_iota(I32, padded, 0)
    across = jnp.broadcast_to(slot, padded)
    down = jnp.sum(jnp.where(lane == sublane, across, zero), 1, keepdims=True)
    place = jnp.sum(jnp.where((across == down) & (lane < sublane), one, zero), 1, keepdims=True)
    place = jnp.where(down == SLOTS, F32(1e6), place)
    column = lax.broadcasted_iota(I32, (1, PADDED), 1)
    base = jnp.zeros((1, 1), F32)
    keep = jnp.ones((1, PADDED), F32)
    last = jnp.zeros((1, PADDED), F32)
    for s in range(SLOTS):
        size = jnp.sum(jnp.where(slot == s, F32(1), F32(0)), 1, keepdims=True)
        runs = jnp.floor((size + (UNIT - 1)) * (1.0 / UNIT))
        place = place + jnp.where(down == s, base * UNIT, F32(0))
        keep = jnp.where((column.astype(F32) == base) & (size > 0), F32(0), keep)
        last = jnp.where(column == s, jnp.where(size > 0, base + runs - 1, F32(RUNS)), last)
        base = base + runs
    found = jnp.where(place == lane.astype(F32), sublane.astype(F32) + 1, zero)
    found = jnp.sum(found, 0, keepdims=True)
    source = jnp.where(found > 0, found - 1, F32(FINE))
    return jnp.concatenate([source, keep, last, jnp.zeros((5, PADDED), F32)], 0).astype(I32)


def coarse_kernel(
    counts, weights_hbm, target_hbm, row_hbm, col_hbm, a_hbm, back, note_out,
    weights, target, a_vmem, row_map, col_map, merged, run_sums, table, order, partial,
    meta_own, meta, via_up, via_down, send_up, send_down, from_down, from_up,
    rows_out, rows_in, pick, placed, note_own, note_in,
    a_got, map_got, order_got,
    y_sent, y_got, meta_sent, meta_got, out_sent, out_got, back_sent, back_got, note_sent, note_got,
):
    steps = FINE // GROUP

    def a_copy(i):
        part = pl.ds(i * GROUP, GROUP)
        return pltpu.make_async_copy(a_hbm.at[part], a_vmem.at[part], a_got.at[i])

    row_copy = pltpu.make_async_copy(row_hbm, row_map.at[pl.ds(0, FINE)], map_got.at[0])
    col_copy = pltpu.make_async_copy(col_hbm, col_map, map_got.at[1])
    small_copies = [
        pltpu.make_async_copy(src, dst, map_got.at[2 + k])
        for k, (src, dst) in enumerate(
            ((target_hbm, target), (weights_hbm, weights))
        )
    ]
    a_copy(0).start()
    for copy in small_copies:
        copy.start()
    col_copy.start()

    w = lax.axis_index("wide")
    y = lax.axis_index("narrow")
    core = lax.rem(w, 2)
    chip = lax.div(w, 2)
    x = lax.div(chip, Z)
    z = lax.rem(chip, Z)
    up, down = lax.rem(y + 1, NARROW), lax.rem(y + NARROW - 1, NARROW)
    far = lax.rem(y + 2, NARROW)

    def remote(src, dst, sent, got, wide, narrow):
        return pltpu.make_async_remote_copy(
            src_ref=src, dst_ref=dst, send_sem=sent, recv_sem=got,
            device_id={"wide": wide, "narrow": narrow},
            device_id_type=pl.DeviceIdType.MESH,
        )

    barrier = pltpu.get_barrier_semaphore()
    for other in (up, down):
        pl.semaphore_signal(barrier, inc=1, device_id={"wide": w, "narrow": other},
                            device_id_type=pl.DeviceIdType.MESH)

    def piece(slot, size, owner):
        return partial.at[pl.ds(slot, size), pl.ds(owner * ROWS, ROWS), :]

    def y_copy(k):
        s = k // 4
        one = pl.ds(s, 1)
        other = pl.ds(HALF + s, 1)
        if k >= 4 * HALF:
            src, dst, narrow = (
                (piece(HALF, HALF, up), from_down.at[pl.ds(HALF, HALF)], up),
                (piece(0, HALF, down), from_up.at[pl.ds(0, HALF)], down),
            )[k - 4 * HALF]
        else:
            src, dst, narrow = (
                (piece(s, 1, far), via_up.at[one], up),
                (piece(HALF + s, 1, far), via_down.at[one], down),
                (send_up.at[one], from_down.at[one], up),
                (send_down.at[one], from_up.at[other], down),
            )[k % 4]
        return remote(src, dst, y_sent.at[k], y_got.at[k], w, narrow)

    near = [lax.rem(z + Z // 2 + k, Z) for k in range(Z)]

    def each_chip(body):
        def visit(d, carry):
            base = lax.rem(x + X // 2 + d, X) * Z
            for k in range(Z):
                body(base + near[k])
            return carry

        lax.fori_loop(0, X, visit, 0)

    def to_rows(send):
        def body(there):
            @pl.when((there != chip) | (core == 0))
            def _():
                send(there).start()

        each_chip(body)

    def greet(there):
        pl.semaphore_signal(barrier, inc=1, device_id={"wide": 2 * there + 1 - core, "narrow": y},
                            device_id_type=pl.DeviceIdType.MESH)

        @pl.when(there != chip)
        def _():
            pl.semaphore_signal(barrier, inc=1, device_id={"wide": 2 * there + core, "narrow": y},
                                device_id_type=pl.DeviceIdType.MESH)

    each_chip(greet)
    row_copy.start()
    for i in range(1, AHEAD):
        a_copy(i).start()
    for copy in small_copies:
        copy.wait()
    lane = lax.broadcasted_iota(I32, (1, BLOCK), 1)
    turn = lax.rem(lane, SLOTS)
    weight_row = jnp.zeros((1, BLOCK), I32)
    for s in range(SLOTS):
        weight_row = jnp.where(turn == s, weights[s], weight_row)
    meta_own[:, :BLOCK] = jnp.full((1, BLOCK), counts[0], I32)
    meta_own[:, BLOCK:] = weight_row

    table[...] = order_table(target[...], counts[0])
    order_copy = pltpu.make_async_copy(table, order, order_got)
    order_copy.start()
    merged[FINE] = jnp.zeros((BLOCK, 2 * BLOCK), BF16)
    row_map[pl.ds(FINE, SLOTS), :] = jnp.zeros((SLOTS, BLOCK), I32)
    run_sums[RUNS] = jnp.zeros((BLOCK, BLOCK), F32)
    sublane = lax.broadcasted_iota(I32, (BLOCK, BLOCK), 0)

    def reduce_group(i, carry):
        a_copy(i).wait()

        @pl.when(i + AHEAD < steps)
        def _():
            a_copy(i + AHEAD).start()

        for j in range(GROUP):
            b = i * GROUP + j
            merged[b] = merged_block(a_vmem[b], col_map[pl.ds(b, 1), :], sublane)
        return carry

    col_copy.wait()
    lax.fori_loop(0, steps, reduce_group, 0)
    row_copy.wait()
    order_copy.wait()

    def add_runs(i, total):
        for k in range(STEP):
            run = i * STEP + k
            at = [jnp.clip(order[0, run * UNIT + u], 0, FINE) for u in range(UNIT)]
            added = jnp.dot(
                jnp.concatenate([picked(row_map[pl.ds(b, 1), :], sublane) for b in at], 1),
                jnp.concatenate([merged[b] for b in at], 0),
                preferred_element_type=F32,
            )
            added = added[:, :BLOCK] + added[:, BLOCK:]
            total = total * order[1, run].astype(F32) + added
            run_sums[run] = total
        return total

    lax.fori_loop(0, RUNS // STEP, add_runs, jnp.zeros((BLOCK, BLOCK), F32))
    for s in range(SLOTS):
        partial[s] = run_sums[jnp.clip(order[2, s], 0, RUNS)]

    pl.semaphore_wait(barrier, WIDE + 1)
    for s in range(HALF):
        y_copy(4 * s).start()
        y_copy(4 * s + 1).start()
    y_copy(4 * HALF).start()
    y_copy(4 * HALF + 1).start()
    to_rows(lambda there: remote(
        meta_own, meta.at[w], meta_sent, meta_got, 2 * there + 1, y))

    for s in range(HALF):
        y_copy(4 * s).wait_recv()
        send_up[s] = via_up[s] + partial[s, pl.ds(up * ROWS, ROWS), :]
        y_copy(4 * s + 2).start()
        y_copy(4 * s + 1).wait_recv()
        send_down[s] = via_down[s] + partial[HALF + s, pl.ds(down * ROWS, ROWS), :]
        y_copy(4 * s + 3).start()

    for k in range(4 * HALF + 2):
        if k >= 4 * HALF or k % 4 > 1:
            y_copy(k).wait_recv()
    for s in range(SLOTS):
        rows_out[:, s, :] = (
            partial[s, pl.ds(y * ROWS, ROWS), :] + from_down[s] + from_up[s]
        )

    to_rows(lambda there: remote(
        rows_out.at[there], rows_in.at[w], out_sent, out_got, 2 * there + 1, y))

    @pl.when(core == 1)
    def _():
        rows_in[w] = rows_out[chip]
        meta[w] = meta_own[...]
        remote(meta.at[pl.ds(0, WIDE - 1)], meta.at[pl.ds(0, WIDE - 1)], meta_sent, meta_got, w - 1, y).wait_recv()
        total = WIDE * SLOTS
        entry = lax.broadcasted_iota(I32, (WIDE, total), 1)
        device = lax.broadcasted_iota(I32, (WIDE, total), 0)
        count = jnp.concatenate([meta[:, 0, :BLOCK]] * (total // BLOCK), 1).astype(F32)
        weight = jnp.concatenate([meta[:, 0, BLOCK:]] * (total // BLOCK), 1).astype(F32)
        owner = lax.div(entry, SLOTS)
        mine = device == owner
        zero = jnp.zeros_like(count)
        count_row = jnp.sum(jnp.where(mine, count, zero), 0, keepdims=True)
        weight_of = jnp.sum(jnp.where(mine, weight, zero), 0, keepdims=True)
        higher = jnp.sum(jnp.where(device >= owner, count, zero), 0, keepdims=True)
        slot = lax.rem(lax.broadcasted_iota(I32, (1, total), 1), SLOTS).astype(F32)
        live = slot < count_row
        goes_to = jnp.where(live, F32(total) - higher + slot, F32(-1))
        first = F32(total) - jnp.max(higher, 1, keepdims=True)
        wide_rows = lax.broadcasted_iota(I32, (total, total), 0).astype(F32)
        pick[...] = jnp.where(wide_rows == goes_to, F32(1), F32(0)).astype(BF16)
        for k in range(2):
            index = (lax.broadcasted_iota(I32, (SLOTS, total), 0) + (2 * chip + k) * SLOTS).astype(F32)
            above = jnp.sum(jnp.where(goes_to > index, weight_of, F32(0)), 1, keepdims=True)
            above = jnp.where(index[:, :1] >= first, above, F32(0))
            diagonal = lax.broadcasted_iota(I32, (SLOTS, BLOCK), 0) == lax.broadcasted_iota(I32, (SLOTS, BLOCK), 1)
            line = jnp.sum(jnp.where(diagonal, above, F32(0)), 0, keepdims=True).astype(I32)
            if k == 0:
                note_own[...] = line
            else:
                note_out[...] = line
        note = remote(note_own, note_in, note_sent, note_got, w - 1, y)
        note.start()
        most = rows_in.at[pl.ds(0, WIDE - 1)]
        remote(most, most, out_sent, out_got, w - 1, y).wait_recv()
        high, low = split(rows_in[...].reshape(WIDE * SLOTS, BLOCK))
        both = jnp.dot(pick[...], jnp.concatenate([high, low], 1), preferred_element_type=F32)
        placed[...] = (both[:, :BLOCK] + both[:, BLOCK:]).reshape(WIDE, SLOTS, BLOCK)
        back[chip] = placed[w]

        def deliver(there):
            remote(placed.at[2 * there], back.at[chip], back_sent, back_got, 2 * there, y).start()

            @pl.when(there != chip)
            def _():
                remote(placed.at[2 * there + 1], back.at[chip], back_sent, back_got, 2 * there + 1, y).start()

        each_chip(deliver)
        few = back.at[pl.ds(0, CHIPS - 1)]
        remote(few, few, back_sent, back_got, w - 1, y).wait_recv()

    @pl.when(core == 0)
    def _():
        remote(back, back, back_sent, back_got, w + 1, y).wait_recv()
        remote(note_in, note_in, note_sent, note_got, w + 1, y).wait_recv()
        note_out[...] = note_in[...]

    for k in range(4 * HALF + 2):
        y_copy(k).wait_send()

    @pl.when(core == 1)
    def _():
        remote(note_own, note_in, note_sent, note_got, w - 1, y).wait_send()
        most = placed.at[pl.ds(0, WIDE - 1)]
        remote(most, most, back_sent, back_got, w - 1, y).wait_send()
        few = rows_out.at[pl.ds(0, CHIPS - 1)]
        remote(few, few, out_sent, out_got, w - 1, y).wait_send()
        some = meta.at[pl.ds(0, CHIPS - 1)]
        remote(some, some, meta_sent, meta_got, w - 1, y).wait_send()

    @pl.when(core == 0)
    def _():
        remote(rows_out, rows_out, out_sent, out_got, w + 1, y).wait_send()
        some = meta.at[pl.ds(0, CHIPS)]
        remote(some, some, meta_sent, meta_got, w + 1, y).wait_send()


def finish_kernel(back, note, coarse, offset):
    for s in range(SLOTS):
        coarse[s] = back[:, s, :]
    offset[...] = note[:, :SLOTS]


def local(a_blocks, row_map, col_map, target, counts, weights):
    vmem = pl.BlockSpec(memory_space=pltpu.VMEM)
    hbm = pl.BlockSpec(memory_space=pltpu.HBM)
    dma = pltpu.SemaphoreType.DMA
    half = pltpu.VMEM((HALF, ROWS, BLOCK), F32)
    full = pltpu.VMEM((SLOTS, ROWS, BLOCK), F32)
    plane = pltpu.VMEM((WIDE, SLOTS, BLOCK), F32)
    line = pltpu.VMEM((1, BLOCK), I32)
    back, note = pl.pallas_call(
        coarse_kernel,
        out_shape=(
            jax.ShapeDtypeStruct((CHIPS, SLOTS, BLOCK), F32),
            jax.ShapeDtypeStruct((1, BLOCK), I32),
        ),
        in_specs=[pl.BlockSpec(memory_space=pltpu.SMEM)] + [hbm] * 5,
        out_specs=(vmem, vmem),
        scratch_shapes=[
            pltpu.SMEM((SLOTS,), I32),
            pltpu.VMEM((1, FINE), I32),
            pltpu.VMEM((FINE, BLOCK, BLOCK), F32),
            pltpu.VMEM((FINE + SLOTS, BLOCK), I32),
            pltpu.VMEM((FINE, BLOCK), I32),
            pltpu.VMEM((FINE + 1, BLOCK, 2 * BLOCK), BF16),
            pltpu.VMEM((RUNS + 1, BLOCK, BLOCK), F32),
            pltpu.VMEM((8, PADDED), I32),
            pltpu.SMEM((8, PADDED), I32),
            pltpu.VMEM((SLOTS, BLOCK, BLOCK), F32),
            pltpu.VMEM((1, 2 * BLOCK), I32),
            pltpu.VMEM((WIDE, 1, 2 * BLOCK), I32),
            half, half, half, half, full, full,
            pltpu.VMEM((CHIPS, SLOTS, BLOCK), F32),
            plane,
            pltpu.VMEM((WIDE * SLOTS, WIDE * SLOTS), BF16),
            plane,
            line, line,
            dma((FINE // GROUP,)), dma((4,)), dma,
            dma((4 * HALF + 2,)), dma((4 * HALF + 2,)),
            dma, dma, dma, dma, dma, dma, dma, dma,
        ],
        compiler_params=pltpu.CompilerParams(
            collective_id=0, has_side_effects=True, vmem_limit_bytes=VMEM_LIMIT
        ),
        name="coarse_blocks",
    )(counts, *(pltpu.with_memory_space_constraint(each, pltpu.HBM) for each in (
        weights, target.reshape(1, FINE), row_map, col_map, a_blocks)))
    coarse, offset = pl.pallas_call(
        finish_kernel,
        out_shape=(
            jax.ShapeDtypeStruct((SLOTS, ROWS, BLOCK), F32),
            jax.ShapeDtypeStruct((1, SLOTS), I32),
        ),
        in_specs=[vmem, vmem],
        out_specs=(vmem, vmem),
        compiler_params=pltpu.CompilerParams(vmem_limit_bytes=4 * 2**20),
        name="finish",
    )(back, note)
    return coarse, offset.reshape(SLOTS)


def solution(mesh):
    return jax.shard_map(
        local,
        mesh=mesh,
        in_specs=(
            P(("wide", "narrow"), None, None),
            P(("wide", "narrow"), None),
            P(("wide", "narrow"), None),
            P(("wide", "narrow")),
            P("wide"),
            P("wide"),
        ),
        out_specs=(P("wide", "narrow", None), P("wide")),
        check_vma=False,
    )
```
